32 devices in a mesh: rep: 4 (over x, y), dp: 8 (over z, core).
Axes of the slice: x: 2, y: 2, z: 4, core: 2. Of those that a mesh axis runs over, the one named last changes fastest.
Arguments:
- g_w_gate: bfloat16 [32, 2, 1280, 4096], P(('rep', 'dp')), parts along dimension 0
- g_w_up: bfloat16 [32, 2, 1280, 4096], P(('rep', 'dp')), parts along dimension 0
- g_w_down: bfloat16 [32, 2, 4096, 1280], P(('rep', 'dp')), parts along dimension 0
- w_gate: bfloat16 [2, 1280, 4096], replicated
- w_up: bfloat16 [2, 1280, 4096], replicated
- w_down: bfloat16 [2, 4096, 1280], replicated
- m_w_gate: float32 [2, 1280, 4096], P(None, 'dp')
- m_w_up: float32 [2, 1280, 4096], P(None, 'dp')
- m_w_down: float32 [2, 4096, 1280], P(None, 'dp')
- v_w_gate: float32 [2, 1280, 4096], P(None, 'dp')
- v_w_up: float32 [2, 1280, 4096], P(None, 'dp')
- v_w_down: float32 [2, 4096, 1280], P(None, 'dp')
Outputs:
- output 1: bfloat16 [8, 1280, 4096], P('rep'), parts along dimension 0
- output 2: bfloat16 [8, 1280, 4096], P('rep'), parts along dimension 0
- output 3: bfloat16 [8, 4096, 1280], P('rep'), parts along dimension 0
- output 4: float32 [8, 1280, 4096], P('rep', 'dp'), parts along dimension 0
- output 5: float32 [8, 1280, 4096], P('rep', 'dp'), parts along dimension 0
- output 6: float32 [8, 4096, 1280], P('rep', 'dp'), parts along dimension 0
- output 7: float32 [8, 1280, 4096], P('rep', 'dp'), parts along dimension 0
- output 8: float32 [8, 1280, 4096], P('rep', 'dp'), parts along dimension 0
- output 9: float32 [8, 4096, 1280], P('rep', 'dp'), parts along dimension 0
There are 4 independent parts. The reference program is written for one: setup_inputs(seed, part) draws one part's arguments, and reference() takes and returns one part's arrays. A program takes and returns all parts, laid end to end along the dimension named above; an argument that names none is the same for every part.
All inputs are finite; a program needn't handle non-finite values.
Results may differ from the reference program's by a relative error of at most 0.022.
Values are sent between devices in bfloat16 or wider.
A program may use at most 2 GiB of HBM per device.

```python
import jax
import jax.numpy as jnp
from jax import lax

DEVICES = 8
D = 1280
FF = 4096
LAYERS = 2
NAMES = ("w_gate", "w_up", "w_down")
SHAPES = {"w_gate": (LAYERS, D, FF), "w_up": (LAYERS, D, FF), "w_down": (LAYERS, FF, D)}


def setup_inputs(seed: int = 0, part: int = 0) -> dict:
    kz, *keys = jax.random.split(jax.random.key(seed), 1 + 5 * len(NAMES))
    loud = 2.0 ** jax.random.uniform(kz, (), jnp.float32, -1.0, 1.0)
    drawn = {}
    for name, key, both in zip(NAMES, keys[:3], keys[3:6], strict=True):
        own = jax.random.normal(jax.random.fold_in(key, part), (DEVICES, *SHAPES[name]), jnp.float32)
        shared = jax.random.normal(jax.random.fold_in(both, part), SHAPES[name], jnp.float32)
        drawn["g_" + name] = (loud * (0.7 * shared / DEVICES + 0.7 * own * DEVICES**-0.5)).astype(jnp.bfloat16)
    for name, key in zip(NAMES, keys[6:9], strict=True):
        drawn[name] = (jax.random.normal(key, SHAPES[name], jnp.float32) * SHAPES[name][1] ** -0.5).astype(jnp.bfloat16)
    for name, key in zip(NAMES, keys[9:12], strict=True):
        drawn["m_" + name] = loud * 0.5 * jax.random.normal(key, SHAPES[name], jnp.float32)
    for name, key in zip(NAMES, keys[12:15], strict=True):
        drawn["v_" + name] = loud * loud * jax.random.uniform(key, SHAPES[name], jnp.float32, 0.5, 1.5)
    return drawn


def adamw(w, m, v, g):
    m = 0.9 * m + 0.1 * g
    v = 0.95 * v + 0.05 * g * g
    step = m * lax.rsqrt(v + 1e-8) + 0.1 * w
    return (w - 0.02 * step).astype(jnp.bfloat16), m, v


def reference(g_w_gate, g_w_up, g_w_down, w_gate, w_up, w_down, m_w_gate, m_w_up, m_w_down, v_w_gate, v_w_up, v_w_down):
    def total(terms):
        return lax.scan(lambda so_far, term: (so_far + term.astype(jnp.float32), None), jnp.zeros(terms.shape[1:], jnp.float32), terms)[0]

    gradients = [total(terms).astype(jnp.bfloat16).astype(jnp.float32) for terms in (g_w_gate, g_w_up, g_w_down)]
    new = [
        adamw(w.astype(jnp.float32), m, v, g)
        for w, m, v, g in zip((w_gate, w_up, w_down), (m_w_gate, m_w_up, m_w_down), (v_w_gate, v_w_up, v_w_down), gradients, strict=True)
    ]
    return tuple(one[which] for which in range(3) for one in new)
```

```python
import functools

import jax
import jax.numpy as jnp
from jax import lax
from jax.experimental import pallas as pl
from jax.experimental.pallas import tpu as pltpu
from jax.sharding import PartitionSpec as P

F32, BF16 = jnp.float32, jnp.bfloat16
MESH = pl.DeviceIdType.MESH
HOP = 3
SHIFT = (HOP - 1) // 2
AHEAD = 4
RING, FAR = 8, 16
ROWS = (16, 64)


def adamw(w, m, v, g):
    m = 0.9 * m + 0.1 * g
    v = 0.95 * v + 0.05 * g * g
    step = m * lax.rsqrt(v + 1e-8) + 0.1 * w
    return (w - 0.02 * step).astype(BF16), m, v


def kernel(*refs):
    grads, weights, m_in, v_in, w_out, m_out, v_out = (refs[i : i + 3] for i in range(0, 21, 3))
    own, par, rcv, snd, fin, wl, ml, vl = (refs[i : i + 2] for i in range(21, 37, 2))
    own_s, par_ss, par_rs, load_s, store_s, rs, ss, both_ss, both_rs = refs[37:]

    layers = m_in[0].shape[0]
    block = [m.shape[1] for m in m_in]
    per = [block[0] // ROWS[0], block[2] // ROWS[1]]
    first_down = 2 * layers * per[0]
    K = first_down + layers * per[1]

    dp = lax.axis_index("dp")
    z, core = dp // 2, dp % 2
    side = z // 2
    edge = (z == 0) | (z == 3)
    middle = jnp.logical_not(edge)
    inner = {"dp": 2 * (z + 1 - 2 * side) + core}
    outer_z = jnp.clip(z - 1 + 2 * side, 0, 3)
    outer = {"dp": 2 * outer_z + core}
    partner = {"dp": 2 * z + 1 - core}

    def owner(b):
        return 2 * (b + side * (3 - 2 * b)) + core

    def other(b):
        return 2 * (b + side * (3 - 2 * b)) + 1 - core

    def by_weight(c, do):
        n = layers * per[0]
        pl.when(c < n)(lambda: do(0, c // per[0], c % per[0]))
        pl.when((c >= n) & (c < 2 * n))(lambda: do(1, (c - n) // per[0], c % per[0]))
        pl.when(c >= 2 * n)(lambda: do(2, (c - 2 * n) // per[1], (c - 2 * n) % per[1]))

    def by_kind(c, do):
        pl.when(c < first_down)(lambda: do(0))
        pl.when(c >= first_down)(lambda: do(1))

    def rows_of(i, device, sub):
        h = ROWS[i // 2]
        return pl.ds(pl.multiple_of(device * block[i] + sub * h, h), h)

    def decode(pos):
        valid = (pos >= 0) & (pos < 4 * K)
        j = pos - (K - SHIFT)
        jc = jnp.maximum(j, 0)
        k, odd = jc // 2, jc % 2 == 1
        head, tail = valid & (j < 0), valid & (pos >= 3 * K + SHIFT)
        mid = valid & (j >= 0) & (pos < 3 * K + SHIFT)
        even = jnp.logical_not(odd)
        is_a = head | (mid & odd & (k < SHIFT))
        is_x = mid & even & (k < K)
        is_y = mid & odd & (k >= SHIFT)
        is_b = tail | (mid & even & (k >= K))
        in_mid = jnp.where(odd, jnp.where(k < SHIFT, K - SHIFT + k, k - SHIFT), jnp.where(k < K, k, k - K))
        return is_a, is_x, is_y, is_b, jnp.where(head, pos, jnp.where(tail, pos - 3 * K, in_mid))

    def pos_f(s):
        return s - jnp.where(edge, 0, HOP)

    def pos_g(s):
        return s - jnp.where(edge, 3 * HOP, 2 * HOP)

    def copy(src, dst, sem):
        return pltpu.make_async_copy(src, dst, sem)

    def remote(src, dst, send, recv, device):
        return pltpu.make_async_remote_copy(src_ref=src, dst_ref=dst, send_sem=send, recv_sem=recv, device_id=device, device_id_type=MESH)


    def tasks(s):
        fa, fx, fy, _, fc = decode(pos_f(s))
        ga, gx, _, _, gc = decode(pos_g(s))
        f_block = jnp.where(fa, 3, jnp.where(fx, 2, 1))
        g_block = jnp.where(ga, 0, 1)
        return ((0, fa | fx | (fy & edge), f_block, fc), (1, ga | (gx & middle), g_block, gc))

    def finals(s):
        ga, gx, _, _, gc = decode(pos_g(s))
        return (ga & edge) | (gx & middle), jnp.where(ga, 0, 1), gc

    def start_loads(s):
        near, far = s % RING, s % FAR
        for stream, wanted, b, c in tasks(s):

            @pl.when(wanted)
            def _(stream=stream, b=b, c=c):
                def go(i, layer, sub):
                    q = i // 2
                    copy(grads[i].at[layer, rows_of(i, owner(b), sub)], own[q].at[stream, near], own_s.at[stream, near]).start()
                    remote(
                        grads[i].at[layer, rows_of(i, other(b), sub)], par[q].at[stream, far],
                        par_ss.at[stream, near], par_rs.at[stream, far], partner,
                    ).start()

                by_weight(c, go)

        done, _, c = finals(s)

        @pl.when(done)
        def _():
            def go(i, layer, sub):
                q, h = i // 2, ROWS[i // 2]
                mine = pl.ds(pl.multiple_of(sub * h, h), h)
                copy(weights[i].at[layer, rows_of(i, dp, sub)], wl[q].at[near], load_s.at[0, near]).start()
                copy(m_in[i].at[layer, mine], ml[q].at[near], load_s.at[1, near]).start()
                copy(v_in[i].at[layer, mine], vl[q].at[near], load_s.at[2, near]).start()

            by_weight(c, go)

    def wait_loads(s, stream, c):
        near, far = s % RING, s % FAR

        def go(q):
            copy(own[q].at[stream, near], own[q].at[stream, near], own_s.at[stream, near]).wait()
            remote(par[q].at[stream, far], par[q].at[stream, far], par_ss.at[stream, near], par_rs.at[stream, far], partner).wait_recv()

        by_kind(c, go)

    def wait_given(s):
        near, far = s % RING, s % FAR
        for stream, wanted, _, c in tasks(s):

            @pl.when(wanted)
            def _(stream=stream, c=c):
                by_kind(c, lambda q: remote(par[q].at[stream, far], par[q].at[stream, far], par_ss.at[stream, near], par_rs.at[stream, far], partner).wait_send())


    def main_sends(s):
        near = s % RING
        pf, pg = pos_f(s), pos_g(s)
        fa, fx, fy, fb, fc = decode(pf)
        ga, gx, gy, gb, gc = decode(pg)
        f_ring = jnp.where(edge, 0, 1)

        def sums(stream):
            return lambda i: snd[i // 2].at[stream, near]

        return (
            ("sum", fa | fx | (fy & edge), fc, 0, inner, f_ring, pf % FAR, None),
            ("new", fy & middle, fc, 0, inner, f_ring, pf % FAR, 1),
            ("old", fb, fc, 0, inner, f_ring, pf % FAR, 0),
            ("sum", ga & middle, gc, 1, outer, 1, pg % FAR, None),
            ("new", gx & middle, gc, 1, outer, 1, pg % FAR, 1),
            ("old", (gy | gb) & middle, gc, 1, outer, 1, pg % FAR, jnp.where(gy, 2, 3)),
        )

    def start_send(s, entry):
        near = s % RING
        what, when, c, stream, device, ring, far, b = entry

        @pl.when(when)
        def _():
            if what == "sum":

                def go(q):
                    remote(snd[q].at[stream, near], rcv[q].at[ring, far], ss.at[stream, near], rs.at[ring, far], device).start()

                by_kind(c, go)
            else:

                def go(i, layer, sub):
                    place = w_out[i].at[layer, rows_of(i, owner(b), sub)]
                    src = fin[i // 2].at[near] if what == "new" else place
                    remote(src, place, ss.at[stream, near], rs.at[ring, far], device).start()

                by_weight(c, go)

    def shares(s):
        fa, fx, fy, fb, fc = decode(pos_f(s))
        ga, gx, gy, gb, gc = decode(pos_g(s))
        done, b, c = finals(s)
        return (
            (done, c, 0, "new", b),
            (fb & middle, fc, 1, "old", 0),
            (gy | gb | (gx & edge), gc, 2, "old", jnp.where(gy, 2, jnp.where(gb, 3, 1))),
        )

    def start_share(s, entry):
        near, far = s % RING, s % FAR
        when, c, which, what, b = entry

        @pl.when(when)
        def _():
            def go(i, layer, sub):
                place = w_out[i].at[layer, rows_of(i, owner(b), sub)]
                src = fin[i // 2].at[near] if what == "new" else place
                remote(src, place, both_ss.at[which, near], both_rs.at[which, far], partner).start()

            by_weight(c, go)

    def some(q):
        return fin[q].at[0]

    def wait_sends(s):
        near, far = s % RING, s % FAR
        for stream, entries in ((0, main_sends(s)[:3]), (1, main_sends(s)[3:])):
            when = functools.reduce(lambda a, b: a | b, [e[1] for e in entries])

            @pl.when(when)
            def _(stream=stream, c=entries[0][2]):
                by_kind(c, lambda q: remote(some(q), some(q), ss.at[stream, near], rs.at[0, 0], inner).wait_send())

        for when, c, which, _, _ in shares(s):

            @pl.when(when)
            def _(c=c, which=which):
                by_kind(c, lambda q: remote(some(q), some(q), both_ss.at[which, near], both_rs.at[which, far], partner).wait_send())

    def wait_shares(s):
        near, far = s % RING, s % FAR
        for when, c, which, _, _ in shares(s):

            @pl.when(when)
            def _(c=c, which=which):
                by_kind(c, lambda q: remote(some(q), some(q), both_ss.at[which, near], both_rs.at[which, far], partner).wait_recv())

    def wait_main(ring, pos, when, c):
        far = pos % FAR

        @pl.when(when)
        def _():
            by_kind(c, lambda q: remote(rcv[q].at[ring, far], rcv[q].at[ring, far], ss.at[0, 0], rs.at[ring, far], inner).wait_recv())

    def tiles(q, do):
        h, n = rcv[q].shape[2:]
        if q == 0:
            width = min(n, 512)

            @pl.loop(0, n // width)
            def _(i):
                do((slice(None), pl.ds(pl.multiple_of(i * width, width), width)))
        else:

            @pl.loop(0, h // 16)
            def _(i):
                do((pl.ds(pl.multiple_of(i * 16, 16), 16), slice(None)))

    def add(s, stream, pos, c, received):
        near, far = s % RING, s % FAR

        def go(q):
            def tile(at):
                total = own[q][(stream, near, *at)].astype(F32) + par[q][(stream, far, *at)].astype(F32)
                if received:
                    total = total + rcv[q][(stream, pos % FAR, *at)].astype(F32)
                snd[q][(stream, near, *at)] = total.astype(BF16)

            tiles(q, tile)

        by_kind(c, go)

    def finish(s, c, both):
        near, far = s % RING, s % FAR
        pf, pg = pos_f(s), pos_g(s)

        def loaded(q):
            for n, buf in enumerate((wl, ml, vl)):
                copy(buf[q].at[near], buf[q].at[near], load_s.at[n, near]).wait()

            def tile(at):
                total = own[q][(1, near, *at)].astype(F32) + par[q][(1, far, *at)].astype(F32)
                total = total + rcv[q][(1, pg % FAR, *at)].astype(F32)
                if both:
                    total = total + rcv[q][(0, pf % FAR, *at)].astype(F32)
                g = total.astype(BF16).astype(F32)
                w, m, v = adamw(wl[q][(near, *at)].astype(F32), ml[q][(near, *at)], vl[q][(near, *at)], g)
                fin[q][(near, *at)] = w
                ml[q][(near, *at)] = m
                vl[q][(near, *at)] = v

            tiles(q, tile)

        by_kind(c, loaded)

    def store(s, c):
        near = s % RING

        def go(i, layer, sub):
            q, h = i // 2, ROWS[i // 2]
            mine = pl.ds(pl.multiple_of(sub * h, h), h)
            copy(fin[q].at[near], w_out[i].at[layer, rows_of(i, dp, sub)], store_s.at[0, near]).start()
            copy(ml[q].at[near], m_out[i].at[layer, mine], store_s.at[1, near]).start()
            copy(vl[q].at[near], v_out[i].at[layer, mine], store_s.at[2, near]).start()

        by_weight(c, go)

    def wait_stores(s):
        near = s % RING
        done, _, c = finals(s)

        @pl.when(done)
        def _():
            def go(q):
                for n, buf in enumerate((fin, ml, vl)):
                    copy(buf[q].at[near], buf[q].at[near], store_s.at[n, near]).wait()

            by_kind(c, go)

    barrier = pltpu.get_barrier_semaphore()
    for device in (inner, partner):
        pl.semaphore_signal(barrier, inc=1, device_id=device, device_id_type=MESH)

    @pl.when(middle)
    def _():
        pl.semaphore_signal(barrier, inc=1, device_id=outer, device_id_type=MESH)
        pl.semaphore_wait(barrier, 3)

    @pl.when(edge)
    def _():
        pl.semaphore_wait(barrier, 2)

    @pl.loop(0, AHEAD)
    def _(s):
        start_loads(s)

    @pl.loop(0, 4 * K + 3 * HOP + 6)
    def _(s):
        pf, pg = pos_f(s), pos_g(s)
        fa, fx, fy, fb, fc = decode(pf)
        ga, gx, gy, gb, gc = decode(pg)
        sends, share = main_sends(s), shares(s)
        wait_stores(s - 2)
        wait_sends(s - 6)
        wait_given(s - 2)
        start_loads(s + AHEAD)
        wait_main(0, pf, (fa | fx | fy | fb) & middle, fc)
        start_send(s, sends[2])
        start_share(s, share[1])
        f_adds = fa | fx | (fy & edge)

        @pl.when(f_adds)
        def _():
            wait_loads(s, 0, fc)
            pl.when(edge)(lambda: add(s, 0, pf, fc, False))
            pl.when(middle)(lambda: add(s, 0, pf, fc, True))

        wait_main(1, pg, ga | gx | gy | gb, gc)
        start_send(s, sends[5])
        start_share(s, share[2])
        start_send(s, sends[0])
        last = (ga & edge) | (gx & middle)

        @pl.when(ga | (gx & middle))
        def _():
            wait_loads(s, 1, gc)

            @pl.when(ga & middle)
            def _():
                add(s, 1, pg, gc, True)

            pl.when(ga & edge)(lambda: finish(s, gc, False))
            pl.when(gx & middle)(lambda: finish(s, gc, True))

        wait_shares(s - 3)
        start_send(s, sends[1])
        start_send(s, sends[3])
        start_send(s, sends[4])
        start_share(s, share[0])
        pl.when(last)(lambda: store(s, gc))


def solution(mesh):
    def step(*arrays):
        terms, weights, m, v = (arrays[i : i + 3] for i in (0, 3, 6, 9))
        shapes = [(ROWS[q], weights[2 * q].shape[2]) for q in (0, 1)]

        def ring(*lead, dtype=BF16):
            return [pltpu.VMEM((*lead, *shape), dtype) for shape in shapes]

        def sems(*shape):
            return pltpu.SemaphoreType.DMA(shape)

        like = lambda x: jax.ShapeDtypeStruct(x.shape, x.dtype)
        anywhere = pl.BlockSpec(memory_space=pl.ANY)
        return pl.pallas_call(
            kernel,
            out_shape=[like(x) for x in (*weights, *m, *v)],
            in_specs=[anywhere] * 12,
            out_specs=[anywhere] * 9,
            scratch_shapes=[
                *ring(2, RING), *ring(2, FAR), *ring(2, FAR), *ring(2, RING), *ring(RING), *ring(RING),
                *ring(RING, dtype=F32), *ring(RING, dtype=F32),
                sems(2, RING), sems(2, RING), sems(2, FAR), sems(3, RING), sems(3, RING), sems(2, FAR), sems(2, RING), sems(3, RING), sems(3, FAR),
            ],
            compiler_params=pltpu.CompilerParams(collective_id=0, has_side_effects=True, vmem_limit_bytes=60 * 2**20),
        )(*(t[0] for t in terms), *weights, *m, *v)

    all_of, cut = P(None, None, None), P(None, "dp", None)
    return jax.shard_map(
        step,
        mesh=mesh,
        in_specs=(P(("rep", "dp"), None, None, None),) * 3 + (all_of,) * 3 + (cut,) * 6,
        out_specs=(P("rep", None, None),) * 3 + (P("rep", "dp", None),) * 6,
        check_vma=False,
    )
```
